32 devices in a mesh: rows: 4 (over x, core), cols: 8 (over z, y).
Axes of the slice: x: 2, y: 2, z: 4, core: 2. Of those that a mesh axis runs over, the one named last changes fastest.
Arguments:
- samples: bfloat16 [2048, 65536], P('rows', 'cols'), may hold values from -0.0234375 to 0.0234375
- labels: int32 [2048], P('rows'), may hold values 0 or 1
- weights: float32 [65536], P('cols'), may hold values from -7 to 7, as said below
- hist_s: float32 [16, 65536], P(None, 'cols'), may hold values from -60 to 60
- hist_y: float32 [16, 65536], P(None, 'cols'), may hold values from -480 to 480, as said below
- counter: int32 [1], replicated, may hold values from 0 to 4095
Outputs:
- new_weights: float32 [65536], P('cols')
- gradient: float32 [65536], P('cols')
The draws below stay inside these ranges and needn't reach their ends.
Inputs may be any that keep to these rules, and one draw needn't show every extreme that they name: weights share a common direction with the rows of hist_s. Each entry of hist_y[j] is a positive multiple of the same entry of hist_s[j], so s_j . y_j > 0.
All inputs are finite; a program needn't handle non-finite values. No bound on the sum of `labels` on one device may be relied on, other than what follows from the above.
Results may differ from the reference program's by a relative error of at most 0.0013.
Values sent between devices are 32-bit elements; how exact they have to be, the bound alone decides.
A program may use at most 64 MiB of HBM per device.

```python
import math
import jax
import jax.numpy as jnp
from jax import lax

FEAT = 65536
HIST = 16
SAMPLES = 2048


def common_base(key):
    return jax.random.truncated_normal(jax.random.fold_in(key, 101), -4.0, 4.0, (FEAT,), jnp.float32)


def draw_weights(key, part):
    base = common_base(key)
    noise = jax.random.truncated_normal(jax.random.fold_in(key, 103), -4.0, 4.0, (FEAT,), jnp.float32)
    return base + 0.5 * noise


def draw_hist_s(key, part):
    base = common_base(key)
    mixing = jax.random.uniform(jax.random.fold_in(key, 107), (HIST, 1), jnp.float32, -1.0, 1.0)
    noise = jax.random.truncated_normal(jax.random.fold_in(key, 109), -4.0, 4.0, (HIST, FEAT), jnp.float32)
    field = mixing * base[None, :] + 0.5 * noise
    return field


def draw_hist_y(key, part):
    field = draw_hist_s(key, part)
    factor = jnp.exp(jax.random.uniform(jax.random.fold_in(key, 127), (HIST, FEAT), jnp.float32, math.log(0.5), math.log(4.0)))
    return factor * field


def touch_ends(array, key, least, top_value):
    longest = array.shape.index(max(array.shape))
    spots = []
    for shift in (0, 1):
        where = [jax.random.randint(jax.random.fold_in(key, axis), (), 0, length) for axis, length in enumerate(array.shape)]
        where[longest] = (where[longest] + shift) % array.shape[longest]
        spots.append(tuple(where))
    return array.at[spots[0]].set(least).at[spots[1]].set(top_value)


def shard_levels(key, dims, shards, low, top_value):
    factor_of, own = 1.0, jax.random.fold_in(key, 6)
    for position, parts in shards:
        steps = jnp.exp(jax.random.uniform(jax.random.fold_in(own, position), (parts,), jnp.float32, low / len(shards), top_value / len(shards)))
        factor_of = factor_of * jnp.repeat(steps, dims[position] // parts).reshape([-1 if axis == position else 1 for axis in range(len(dims))])
    return factor_of


def scatter_about(rng, extent, scale, limit, cuts=(), held_as=jnp.bfloat16):
    factor_of = shard_levels(rng, extent, cuts, -0.22, 0.18) if cuts else 1.0
    drawn = jax.random.normal(rng, extent, jnp.float32) * scale * factor_of
    return jnp.minimum(jnp.maximum(drawn, -limit), limit).astype(held_as)


def setup_inputs(seed: int = 0) -> dict:
    key_list = jax.random.split(jax.random.key(seed), 7)
    samples = scatter_about(key_list[0], (SAMPLES, FEAT), FEAT ** -0.5, 0.0234375, ((0, 4), (1, 8)))
    labels = touch_ends((jax.random.randint(key_list[1], (SAMPLES,), 0, 2) < 1).astype(jnp.int32), jax.random.fold_in(key_list[1], 1), 0, 1)
    weights = draw_weights(jax.random.fold_in(key_list[6], 71), 0)
    hist_s = draw_hist_s(jax.random.fold_in(key_list[6], 71), 0)
    hist_y = draw_hist_y(jax.random.fold_in(key_list[6], 71), 0)
    counter = jax.random.randint(key_list[5], (1,), 0, 4096).astype(jnp.int32)
    return {"samples": samples, "labels": labels, "weights": weights, "hist_s": hist_s, "hist_y": hist_y, "counter": counter}


penalty = 4.0
step_length = 0.5


def pick(table, slot):
    return lax.dynamic_index_in_dim(table, slot, 0, keepdims=False)


def reference(samples, labels, weights, hist_s, hist_y, counter):
    margin = jnp.dot(samples, weights.astype(jnp.bfloat16), preferred_element_type=jnp.float32)
    resid = (jax.nn.sigmoid(margin) - labels.astype(jnp.float32)).astype(jnp.bfloat16)
    total = jnp.dot(resid, samples, preferred_element_type=jnp.float32)
    gradient = weights + penalty * total
    newest = (counter[0] % HIST).astype(jnp.int32)
    curv = jnp.sum(hist_s * hist_y, axis=1)
    rho = 1.0 / curv
    y_new = pick(hist_y, newest)
    gamma = pick(curv, newest) / jnp.sum(y_new * y_new)
    query = gradient
    coefs = []
    slots = []
    for step in range(HIST):
        slot = ((newest - step) % HIST).astype(jnp.int32)
        slots.append(slot)
        coef = pick(rho, slot) * jnp.sum(pick(hist_s, slot) * query)
        coefs.append(coef)
        query = query - coef * pick(hist_y, slot)
    result = gamma * query
    for step in reversed(range(HIST)):
        slot = slots[step]
        beta = pick(rho, slot) * jnp.sum(pick(hist_y, slot) * result)
        result = result + (coefs[step] - beta) * pick(hist_s, slot)
    return weights - step_length * result, gradient
```

```python
import functools

import jax
import jax.numpy as jnp
from jax import lax
from jax.experimental import pallas as pl
from jax.experimental.pallas import tpu as pltpu
from jax.sharding import PartitionSpec as P

HIST = 16
LANES = 128
LOAD_CHUNKS = 8
SEND_CHUNKS = 4

penalty = 4.0
step_length = 0.5
highest = lax.Precision.HIGHEST
f32 = jnp.float32
bf16 = jnp.bfloat16


def dot_nt(left, right, precision=None):
    return lax.dot_general(
        left, right, (((1,), (1,)), ((), ())), precision=precision, preferred_element_type=f32
    )


def split(values):
    high = values.astype(bf16)
    rest = values - high.astype(f32)
    return high, rest


def iota(shape, dim):
    return lax.broadcasted_iota(jnp.int32, shape, dim)


def kernel(
    rows, cols,
    counter_ref, labels_ref, samples_hbm, weights_hbm, s_hbm, y_hbm,
    out_ref, grad_ref,
    samples, weights, hist, basis, gram_slots, margin_slots, dot_slots, total_slots,
    load_sem, hist_sem, gram_send, gram_recv, margin_send, margin_recv,
    dot_send, dot_recv, total_send, total_recv,
):
    my_row, my_col = lax.axis_index("rows"), lax.axis_index("cols")
    count = rows * cols
    my_place = my_row * cols + my_col
    feat = samples.shape[1]
    wide = feat // LOAD_CHUNKS
    part = feat // SEND_CHUNKS

    first = [
        pltpu.make_async_copy(s_hbm, hist.at[pl.ds(0, HIST)], hist_sem.at[0]),
        pltpu.make_async_copy(y_hbm, hist.at[pl.ds(HIST, HIST)], hist_sem.at[1]),
        pltpu.make_async_copy(weights_hbm, weights, hist_sem.at[2]),
    ]
    loads = [
        pltpu.make_async_copy(
            samples_hbm.at[:, pl.ds(c * wide, wide)],
            samples.at[:, pl.ds(c * wide, wide)],
            load_sem.at[c],
        )
        for c in range(LOAD_CHUNKS)
    ]
    for copy in first + loads:
        copy.start()

    barrier = pltpu.get_barrier_semaphore()

    def greet(k, carry):
        place = lax.rem(my_place + k, count)
        pl.semaphore_signal(
            barrier, inc=1, device_id=(place // cols, lax.rem(place, cols)),
            device_id_type=pl.DeviceIdType.MESH,
        )
        return carry

    lax.fori_loop(1, count, greet, 0)

    for copy in first:
        copy.wait()
    for c in range(LOAD_CHUNKS):
        at = pl.ds(c * wide, wide)
        high, rest = split(hist[:, at])
        basis[0:32, at] = high
        basis[32:64, at] = rest.astype(bf16)
        w_high, w_rest = split(weights[:, at])
        w_mid, w_rest = split(w_rest)
        line = iota((16, wide), 0)
        block = jnp.where(line == 0, w_high.astype(f32), 0.0)
        block = jnp.where(line == 1, w_mid.astype(f32), block)
        block = jnp.where(line == 2, w_rest, block)
        basis[64:80, at] = block.astype(bf16)
        basis[80:128, at] = jnp.zeros((48, wide), bf16)

    gram = dot_nt(basis[0:80, :], basis[...])
    gram_y = gram[16:32] + gram[48:64]
    gram_y = gram_y + pltpu.roll(gram_y, LANES - 32, 1)
    w_line = jnp.sum(gram[64:80], axis=0, keepdims=True)
    w_line = w_line + pltpu.roll(w_line, LANES - 32, 1)
    gram_slots[my_col] = gram_y

    pl.semaphore_wait(barrier, count - 1)

    def over_cols(slots, send, recv):
        def copy_to(k):
            place = lax.rem(my_col + k, cols)
            return pltpu.make_async_remote_copy(
                src_ref=slots.at[my_col], dst_ref=slots.at[my_col],
                send_sem=send.at[k], recv_sem=recv.at[my_col],
                device_id=(my_row, place), device_id_type=pl.DeviceIdType.MESH,
            )

        def copy_from(k):
            place = lax.rem(my_col + k, cols)
            return pltpu.make_async_remote_copy(
                src_ref=slots.at[place], dst_ref=slots.at[place],
                send_sem=send.at[k], recv_sem=recv.at[place],
                device_id=(my_row, place), device_id_type=pl.DeviceIdType.MESH,
            )

        return copy_to, copy_from

    gram_to, gram_from = over_cols(gram_slots, gram_send, gram_recv)
    margin_to, margin_from = over_cols(margin_slots, margin_send, margin_recv)
    for k in range(1, cols):
        gram_to(k).start()

    product = None
    for c in range(LOAD_CHUNKS):
        at = pl.ds(c * wide, wide)
        loads[c].wait()
        term = dot_nt(basis[0:80, at], samples[:, at])
        product = term if product is None else product + term
    margin_slots[my_col] = product[64:65]
    for k in range(1, cols):
        margin_to(k).start()
    projected = product[0:32] + product[32:64]

    for k in range(1, cols):
        gram_from(k).wait_recv()
    gram = gram_slots[0]
    for k in range(1, cols):
        gram = gram + gram_slots[k]
    newest = lax.rem(counter_ref[0], HIST)
    line, lane = iota((HIST, LANES), 0), iota((HIST, LANES), 1)
    small = lane < HIST
    eye = line == lane
    age_line = lax.rem(newest - line + HIST, HIST)
    age_lane = lax.rem(newest - lane + LANES, HIST)
    sy = jnp.where(small, gram, 0.0)
    yy = jnp.where(small, pltpu.roll(gram, LANES - HIST, 1), 0.0)
    diagonal = jnp.where(eye, sy, 0.0)
    rho_line = 1.0 / jnp.sum(diagonal, axis=1, keepdims=True)
    diag_lane = jnp.sum(diagonal, axis=0, keepdims=True)
    rho_lane = 1.0 / jnp.where(small[0:1], diag_lane, 1.0)
    at_newest = jnp.logical_and(eye, line == newest)
    gamma = jnp.sum(
        jnp.sum(jnp.where(at_newest, sy, 0.0), axis=1, keepdims=True), axis=0, keepdims=True
    ) / jnp.sum(
        jnp.sum(jnp.where(at_newest, yy, 0.0), axis=1, keepdims=True), axis=0, keepdims=True
    )
    strict = jnp.logical_and(small, age_lane > age_line)
    factor = jnp.where(strict, sy * rho_lane, 0.0)
    solved = jnp.where(eye, 1.0, 0.0)
    columns = [
        jnp.sum(jnp.where(age_lane == age, factor, 0.0), axis=1, keepdims=True)
        for age in range(HIST)
    ]
    for age in reversed(range(1, HIST)):
        row = jnp.sum(jnp.where(age_line == age, solved, 0.0), axis=0, keepdims=True)
        solved = solved - columns[age] * row
    solved = solved * rho_line
    tall = lambda block: jnp.concatenate([block, jnp.zeros((LANES - HIST, LANES), f32)], axis=0)
    middle = diagonal + gamma * yy
    inverse = dot_nt(jnp.where(eye, 1.0, 0.0), tall(solved), highest)
    half = dot_nt(middle, tall(solved), highest)
    lower = jnp.dot(solved, tall(half), precision=highest, preferred_element_type=f32)
    map_y = -gamma * inverse
    map_s = lower - gamma * pltpu.roll(solved, HIST, 1)

    labels = labels_ref[...].astype(f32)
    for k in range(1, cols):
        margin_from(k).wait_recv()
    margin = margin_slots[0]
    for k in range(1, cols):
        margin = margin + margin_slots[k]
    resid = (jax.nn.sigmoid(margin) - labels).astype(bf16)
    resid_wide = resid.astype(f32)
    dots = jnp.sum(projected * resid_wide, axis=1, keepdims=True)
    spread = jnp.where(iota((32, LANES), 0) == iota((32, LANES), 1), dots, 0.0)
    dot_slots[my_place] = penalty * jnp.sum(spread, axis=0, keepdims=True) + w_line * (1.0 / rows)

    def dot_copy(k, owner):
        place = lax.rem(my_place + k, count)
        slot = my_place if owner else place
        return pltpu.make_async_remote_copy(
            src_ref=dot_slots.at[slot], dst_ref=dot_slots.at[slot],
            send_sem=dot_send.at[k], recv_sem=dot_recv.at[slot],
            device_id=(place // cols, lax.rem(place, cols)),
            device_id_type=pl.DeviceIdType.MESH,
        )

    def dot_start(k, carry):
        dot_copy(k, True).start()
        return carry

    lax.fori_loop(1, count, dot_start, 0)

    def total_copy(k, c, owner):
        place = lax.rem(my_row + k, rows)
        slot = my_row if owner else place
        return pltpu.make_async_remote_copy(
            src_ref=total_slots.at[slot, c], dst_ref=total_slots.at[slot, c],
            send_sem=total_send.at[k, c], recv_sem=total_recv.at[slot, c],
            device_id=(place, my_col), device_id_type=pl.DeviceIdType.MESH,
        )

    resid_rows = jnp.broadcast_to(resid_wide, (16, resid.shape[1])).astype(bf16)
    for c in range(SEND_CHUNKS):
        at = pl.ds(c * part, part)
        total = jnp.dot(resid_rows, samples[:, at], preferred_element_type=f32)
        total_slots[my_row, c] = total[0:1]
        for k in range(1, rows):
            total_copy(k, c, True).start()

    def dot_wait(k, carry):
        dot_copy(k, False).wait_recv()
        return carry

    lax.fori_loop(1, count, dot_wait, 0)
    inner = jnp.sum(dot_slots[...], axis=0)
    inner = jnp.where(iota((1, LANES), 1) < 32, inner, 0.0)
    coef_y = jnp.sum(map_y * inner, axis=1, keepdims=True)
    coef_s = jnp.sum(map_s * inner, axis=1, keepdims=True)
    for c in range(SEND_CHUNKS):
        at = pl.ds(c * part, part)
        mixed = jnp.sum(
            coef_s * hist[0:16, at] + coef_y * hist[16:32, at], axis=0, keepdims=True
        )
        for k in range(1, rows):
            total_copy(k, c, False).wait_recv()
        total = total_slots[0, c]
        for k in range(1, rows):
            total = total + total_slots[k, c]
        w = weights[:, at]
        gradient = w + penalty * total
        grad_ref[:, at] = gradient
        out_ref[:, at] = w - step_length * (gamma * gradient + mixed)

    for k in range(1, cols):
        gram_to(k).wait_send()
        margin_to(k).wait_send()

    def dot_sent(k, carry):
        dot_copy(k, True).wait_send()
        return carry

    lax.fori_loop(1, count, dot_sent, 0)
    for c in range(SEND_CHUNKS):
        for k in range(1, rows):
            total_copy(k, c, True).wait_send()


def body(rows, cols, samples, labels, weights, hist_s, hist_y, counter):
    height, feat = samples.shape
    count = rows * cols
    dma = pltpu.SemaphoreType.DMA
    anywhere = pl.BlockSpec(memory_space=pl.ANY)
    vmem = pl.BlockSpec(memory_space=pltpu.VMEM)
    new_weights, gradient = pl.pallas_call(
        functools.partial(kernel, rows, cols),
        out_shape=[jax.ShapeDtypeStruct((1, feat), f32)] * 2,
        in_specs=[pl.BlockSpec(memory_space=pltpu.SMEM), vmem] + [anywhere] * 4,
        out_specs=[vmem, vmem],
        scratch_shapes=[
            pltpu.VMEM((height, feat), bf16),
            pltpu.VMEM((1, feat), f32),
            pltpu.VMEM((2 * HIST, feat), f32),
            pltpu.VMEM((LANES, feat), bf16),
            pltpu.VMEM((cols, HIST, LANES), f32),
            pltpu.VMEM((cols, 1, height), f32),
            pltpu.VMEM((count, 1, LANES), f32),
            pltpu.VMEM((rows, SEND_CHUNKS, 1, feat // SEND_CHUNKS), f32),
            dma((LOAD_CHUNKS,)),
            dma((3,)),
            dma((cols,)),
            dma((cols,)),
            dma((cols,)),
            dma((cols,)),
            dma((count,)),
            dma((count,)),
            dma((rows, SEND_CHUNKS)),
            dma((rows, SEND_CHUNKS)),
        ],
        compiler_params=pltpu.CompilerParams(
            collective_id=0, has_side_effects=True, vmem_limit_bytes=60 * 1024 * 1024
        ),
    )(counter, labels.reshape(1, height), samples, weights.reshape(1, feat), hist_s, hist_y)
    return new_weights.reshape(feat), gradient.reshape(feat)


def solution(mesh):
    in_specs = (P("rows", "cols"), P("rows"), P("cols"), P(None, "cols"), P(None, "cols"), P())
    out_specs = (P("cols"), P("cols"))
    run = functools.partial(body, mesh.shape["rows"], mesh.shape["cols"])
    return jax.shard_map(run, mesh=mesh, in_specs=in_specs, out_specs=out_specs, check_vma=False)
```

```python
import functools

import jax
import jax.numpy as jnp
from jax import lax
from jax.experimental import pallas as pl
from jax.experimental.pallas import tpu as pltpu
from jax.sharding import PartitionSpec as P

HIST = 16
LANES = 128
LOAD_CHUNKS = 8
SEND_CHUNKS = 4

penalty = 4.0
step_length = 0.5
highest = lax.Precision.HIGHEST
f32 = jnp.float32
bf16 = jnp.bfloat16


def dot_nt(left, right, precision=None):
    return lax.dot_general(
        left, right, (((1,), (1,)), ((), ())), precision=precision, preferred_element_type=f32
    )


def split(values):
    high = values.astype(bf16)
    rest = values - high.astype(f32)
    return high, rest


def iota(shape, dim):
    return lax.broadcasted_iota(jnp.int32, shape, dim)


def kernel(
    rows, cols,
    counter_ref, labels_ref, samples_hbm, weights_hbm, s_hbm, y_hbm,
    out_ref, grad_ref,
    samples, weights, hist, basis, gram_slots, margin_slots, dot_slots, total_slots,
    load_sem, hist_sem, gram_send, gram_recv, margin_send, margin_recv,
    dot_send, dot_recv, total_send, total_recv,
):
    my_row, my_col = lax.axis_index("rows"), lax.axis_index("cols")
    count = rows * cols
    my_place = my_row * cols + my_col
    feat = samples.shape[1]
    wide = feat // LOAD_CHUNKS
    part = feat // SEND_CHUNKS

    first = [
        pltpu.make_async_copy(s_hbm, hist.at[pl.ds(0, HIST)], hist_sem.at[0]),
        pltpu.make_async_copy(y_hbm, hist.at[pl.ds(HIST, HIST)], hist_sem.at[1]),
        pltpu.make_async_copy(weights_hbm, weights, hist_sem.at[2]),
    ]
    loads = [
        pltpu.make_async_copy(
            samples_hbm.at[:, pl.ds(c * wide, wide)],
            samples.at[:, pl.ds(c * wide, wide)],
            load_sem.at[c],
        )
        for c in range(LOAD_CHUNKS)
    ]
    for copy in first + loads:
        copy.start()

    barrier = pltpu.get_barrier_semaphore()

    def greet(k, carry):
        place = lax.rem(my_place + k, count)
        pl.semaphore_signal(
            barrier, inc=1, device_id=(place // cols, lax.rem(place, cols)),
            device_id_type=pl.DeviceIdType.MESH,
        )
        return carry

    lax.fori_loop(1, count, greet, 0)

    for copy in first:
        copy.wait()

    def over_cols(slots, send, recv):
        def copy_to(k):
            place = lax.rem(my_col + k, cols)
            return pltpu.make_async_remote_copy(
                src_ref=slots.at[my_col], dst_ref=slots.at[my_col],
                send_sem=send.at[k], recv_sem=recv.at[my_col],
                device_id=(my_row, place), device_id_type=pl.DeviceIdType.MESH,
            )

        def copy_from(k):
            place = lax.rem(my_col + k, cols)
            return pltpu.make_async_remote_copy(
                src_ref=slots.at[place], dst_ref=slots.at[place],
                send_sem=send.at[k], recv_sem=recv.at[place],
                device_id=(my_row, place), device_id_type=pl.DeviceIdType.MESH,
            )

        return copy_to, copy_from

    gram_to, gram_from = over_cols(gram_slots, gram_send, gram_recv)
    margin_to, margin_from = over_cols(margin_slots, margin_send, margin_recv)
    product = gram = None
    for c in range(LOAD_CHUNKS):
        at = pl.ds(c * wide, wide)
        high, rest = split(hist[:, at])
        basis[0:32, at] = high
        basis[32:64, at] = rest.astype(bf16)
        w_high, w_rest = split(weights[:, at])
        w_mid, w_rest = split(w_rest)
        line = iota((16, wide), 0)
        block = jnp.where(line == 0, w_high.astype(f32), 0.0)
        block = jnp.where(line == 1, w_mid.astype(f32), block)
        block = jnp.where(line == 2, w_rest, block)
        basis[64:80, at] = block.astype(bf16)
        basis[80:128, at] = jnp.zeros((48, wide), bf16)
        term = dot_nt(basis[0:80, at], basis[:, at])
        gram = term if gram is None else gram + term
        loads[c].wait()
        term = dot_nt(basis[0:80, at], samples[:, at])
        product = term if product is None else product + term
    pl.semaphore_wait(barrier, count - 1)
    margin_slots[my_col] = product[64:65]
    for k in range(1, cols):
        margin_to(k).start()
    gram_y = gram[16:32] + gram[48:64]
    gram_y = gram_y + pltpu.roll(gram_y, LANES - 32, 1)
    w_line = jnp.sum(gram[64:80], axis=0, keepdims=True)
    w_line = w_line + pltpu.roll(w_line, LANES - 32, 1)
    gram_slots[my_col] = gram_y
    for k in range(1, cols):
        gram_to(k).start()
    projected = product[0:32] + product[32:64]

    labels = labels_ref[...].astype(f32)
    for k in range(1, cols):
        margin_from(k).wait_recv()
    margin = margin_slots[0]
    for k in range(1, cols):
        margin = margin + margin_slots[k]
    resid = (jax.nn.sigmoid(margin) - labels).astype(bf16)
    resid_wide = resid.astype(f32)
    dots = jnp.sum(projected * resid_wide, axis=1, keepdims=True)
    spread = jnp.where(iota((32, LANES), 0) == iota((32, LANES), 1), dots, 0.0)
    dot_slots[my_place] = penalty * jnp.sum(spread, axis=0, keepdims=True) + w_line * (1.0 / rows)

    def dot_copy(k, owner):
        place = lax.rem(my_place + k, count)
        slot = my_place if owner else place
        return pltpu.make_async_remote_copy(
            src_ref=dot_slots.at[slot], dst_ref=dot_slots.at[slot],
            send_sem=dot_send.at[k], recv_sem=dot_recv.at[slot],
            device_id=(place // cols, lax.rem(place, cols)),
            device_id_type=pl.DeviceIdType.MESH,
        )

    def dot_start(k, carry):
        dot_copy(k, True).start()
        return carry

    lax.fori_loop(1, count, dot_start, 0)

    def total_copy(k, c, owner):
        place = lax.rem(my_row + k, rows)
        slot = my_row if owner else place
        return pltpu.make_async_remote_copy(
            src_ref=total_slots.at[slot, c], dst_ref=total_slots.at[slot, c],
            send_sem=total_send.at[k, c], recv_sem=total_recv.at[slot, c],
            device_id=(place, my_col), device_id_type=pl.DeviceIdType.MESH,
        )

    resid_rows = jnp.broadcast_to(resid_wide, (16, resid.shape[1])).astype(bf16)
    for c in range(SEND_CHUNKS):
        at = pl.ds(c * part, part)
        total = jnp.dot(resid_rows, samples[:, at], preferred_element_type=f32)
        total_slots[my_row, c] = total[0:1]
        for k in range(1, rows):
            total_copy(k, c, True).start()

    for k in range(1, cols):
        gram_from(k).wait_recv()
    gram = gram_slots[0]
    for k in range(1, cols):
        gram = gram + gram_slots[k]
    newest = lax.rem(counter_ref[0], HIST)
    line, lane = iota((HIST, LANES), 0), iota((HIST, LANES), 1)
    small = lane < HIST
    eye = line == lane
    age_line = lax.rem(newest - line + HIST, HIST)
    age_lane = lax.rem(newest - lane + LANES, HIST)
    sy = jnp.where(small, gram, 0.0)
    yy = jnp.where(small, pltpu.roll(gram, LANES - HIST, 1), 0.0)
    diagonal = jnp.where(eye, sy, 0.0)
    rho_line = 1.0 / jnp.sum(diagonal, axis=1, keepdims=True)
    diag_lane = jnp.sum(diagonal, axis=0, keepdims=True)
    rho_lane = 1.0 / jnp.where(small[0:1], diag_lane, 1.0)
    at_newest = jnp.logical_and(eye, line == newest)
    gamma = jnp.sum(
        jnp.sum(jnp.where(at_newest, sy, 0.0), axis=1, keepdims=True), axis=0, keepdims=True
    ) / jnp.sum(
        jnp.sum(jnp.where(at_newest, yy, 0.0), axis=1, keepdims=True), axis=0, keepdims=True
    )
    strict = jnp.logical_and(small, age_lane > age_line)
    factor = jnp.where(strict, sy * rho_lane, 0.0)
    solved = jnp.where(eye, 1.0, 0.0)
    columns = [
        jnp.sum(jnp.where(age_lane == age, factor, 0.0), axis=1, keepdims=True)
        for age in range(HIST)
    ]
    for age in reversed(range(1, HIST)):
        row = jnp.sum(jnp.where(age_line == age, solved, 0.0), axis=0, keepdims=True)
        solved = solved - columns[age] * row
    solved = solved * rho_line
    tall = lambda block: jnp.concatenate([block, jnp.zeros((LANES - HIST, LANES), f32)], axis=0)
    middle = diagonal + gamma * yy
    inverse = dot_nt(jnp.where(eye, 1.0, 0.0), tall(solved), highest)
    half = dot_nt(middle, tall(solved), highest)
    lower = jnp.dot(solved, tall(half), precision=highest, preferred_element_type=f32)
    map_y = -gamma * inverse
    map_s = lower - gamma * pltpu.roll(solved, HIST, 1)

    def dot_wait(k, carry):
        dot_copy(k, False).wait_recv()
        return carry

    lax.fori_loop(1, count, dot_wait, 0)
    inner = jnp.sum(dot_slots[...], axis=0)
    inner = jnp.where(iota((1, LANES), 1) < 32, inner, 0.0)
    coef_y = jnp.sum(map_y * inner, axis=1, keepdims=True)
    coef_s = jnp.sum(map_s * inner, axis=1, keepdims=True)
    for c in range(SEND_CHUNKS):
        at = pl.ds(c * part, part)
        mixed = jnp.sum(
            coef_s * hist[0:16, at] + coef_y * hist[16:32, at], axis=0, keepdims=True
        )
        for k in range(1, rows):
            total_copy(k, c, False).wait_recv()
        total = total_slots[0, c]
        for k in range(1, rows):
            total = total + total_slots[k, c]
        total = penalty * total
        grad_ref[:, at] = total
        out_ref[:, at] = -step_length * (gamma * (weights[:, at] + total) + mixed)

    for k in range(1, cols):
        gram_to(k).wait_send()
        margin_to(k).wait_send()

    def dot_sent(k, carry):
        dot_copy(k, True).wait_send()
        return carry

    lax.fori_loop(1, count, dot_sent, 0)
    for c in range(SEND_CHUNKS):
        for k in range(1, rows):
            total_copy(k, c, True).wait_send()


def body(rows, cols, samples, labels, weights, hist_s, hist_y, counter):
    height, feat = samples.shape
    count = rows * cols
    dma = pltpu.SemaphoreType.DMA
    anywhere = pl.BlockSpec(memory_space=pl.ANY)
    vmem = pl.BlockSpec(memory_space=pltpu.VMEM)
    direction, total = pl.pallas_call(
        functools.partial(kernel, rows, cols),
        out_shape=[jax.ShapeDtypeStruct((1, feat), f32)] * 2,
        in_specs=[pl.BlockSpec(memory_space=pltpu.SMEM), vmem] + [anywhere] * 4,
        out_specs=[vmem, vmem],
        scratch_shapes=[
            pltpu.VMEM((height, feat), bf16),
            pltpu.VMEM((1, feat), f32),
            pltpu.VMEM((2 * HIST, feat), f32),
            pltpu.VMEM((LANES, feat), bf16),
            pltpu.VMEM((cols, HIST, LANES), f32),
            pltpu.VMEM((cols, 1, height), f32),
            pltpu.VMEM((count, 1, LANES), f32),
            pltpu.VMEM((rows, SEND_CHUNKS, 1, feat // SEND_CHUNKS), f32),
            dma((LOAD_CHUNKS,)),
            dma((3,)),
            dma((cols,)),
            dma((cols,)),
            dma((cols,)),
            dma((cols,)),
            dma((count,)),
            dma((count,)),
            dma((rows, SEND_CHUNKS)),
            dma((rows, SEND_CHUNKS)),
        ],
        compiler_params=pltpu.CompilerParams(
            collective_id=0, has_side_effects=True, vmem_limit_bytes=60 * 1024 * 1024
        ),
    )(counter, labels.reshape(1, height), samples, weights.reshape(1, feat), hist_s, hist_y)
    direction, total = direction.reshape(feat), total.reshape(feat)
    return weights + direction, weights + total


def solution(mesh):
    in_specs = (P("rows", "cols"), P("rows"), P("cols"), P(None, "cols"), P(None, "cols"), P())
    out_specs = (P("cols"), P("cols"))
    run = functools.partial(body, mesh.shape["rows"], mesh.shape["cols"])
    return jax.shard_map(run, mesh=mesh, in_specs=in_specs, out_specs=out_specs, check_vma=False)
```

```python
import functools

import jax
import jax.numpy as jnp
from jax import lax
from jax.experimental import pallas as pl
from jax.experimental.pallas import tpu as pltpu
from jax.sharding import PartitionSpec as P

HIST = 16
LANES = 128
LOAD_CHUNKS = 16
SEND_CHUNKS = 4

penalty = 4.0
step_length = 0.5
highest = lax.Precision.HIGHEST
f32 = jnp.float32
bf16 = jnp.bfloat16


def dot_nt(left, right, precision=None):
    return lax.dot_general(
        left, right, (((1,), (1,)), ((), ())), precision=precision, preferred_element_type=f32
    )


def split(values):
    high = values.astype(bf16)
    rest = values - high.astype(f32)
    return high, rest


def iota(shape, dim):
    return lax.broadcasted_iota(jnp.int32, shape, dim)


def kernel(
    rows, cols,
    counter_ref, labels_hbm, samples_hbm, weights_hbm, s_hbm, y_hbm,
    out_ref, grad_ref,
    labels_ref, samples, weights, hist, basis, gram_slots, margin_slots, dot_slots, total_slots,
    load_sem, hist_sem, gram_send, gram_recv, margin_send, margin_recv,
    dot_send, dot_recv, total_send, total_recv,
):
    my_row, my_col = lax.axis_index("rows"), lax.axis_index("cols")
    count = rows * cols
    my_place = my_row * cols + my_col
    feat = samples.shape[1]
    wide = feat // LOAD_CHUNKS
    part = feat // SEND_CHUNKS

    first = [
        pltpu.make_async_copy(s_hbm, hist.at[pl.ds(0, HIST)], hist_sem.at[0]),
        pltpu.make_async_copy(y_hbm, hist.at[pl.ds(HIST, HIST)], hist_sem.at[1]),
        pltpu.make_async_copy(weights_hbm, weights, hist_sem.at[2]),
    ]
    loads = [
        pltpu.make_async_copy(
            samples_hbm.at[:, pl.ds(c * wide, wide)],
            samples.at[:, pl.ds(c * wide, wide)],
            load_sem.at[c],
        )
        for c in range(LOAD_CHUNKS)
    ]
    label_copy = pltpu.make_async_copy(labels_hbm, labels_ref, hist_sem.at[3])
    for copy in first + loads + [label_copy]:
        copy.start()

    barrier = pltpu.get_barrier_semaphore()

    def greet(k, carry):
        place = lax.rem(my_place + k, count)
        pl.semaphore_signal(
            barrier, inc=1, device_id=(place // cols, lax.rem(place, cols)),
            device_id_type=pl.DeviceIdType.MESH,
        )
        return carry

    lax.fori_loop(1, count, greet, 0)

    for copy in first:
        copy.wait()

    def over_cols(slots, send, recv):
        def copy_to(k):
            place = lax.rem(my_col + k, cols)
            return pltpu.make_async_remote_copy(
                src_ref=slots.at[my_col], dst_ref=slots.at[my_col],
                send_sem=send.at[k], recv_sem=recv.at[my_col],
                device_id=(my_row, place), device_id_type=pl.DeviceIdType.MESH,
            )

        def copy_from(k):
            place = lax.rem(my_col + k, cols)
            return pltpu.make_async_remote_copy(
                src_ref=slots.at[place], dst_ref=slots.at[place],
                send_sem=send.at[k], recv_sem=recv.at[place],
                device_id=(my_row, place), device_id_type=pl.DeviceIdType.MESH,
            )

        return copy_to, copy_from

    gram_to, gram_from = over_cols(gram_slots, gram_send, gram_recv)
    margin_to, margin_from = over_cols(margin_slots, margin_send, margin_recv)
    product = None
    for c in range(LOAD_CHUNKS):
        at = pl.ds(c * wide, wide)
        high, rest = split(hist[:, at])
        basis[0:32, at] = high
        basis[32:64, at] = rest.astype(bf16)
        w_high, w_rest = split(weights[:, at])
        w_mid, w_rest = split(w_rest)
        line = iota((16, wide), 0)
        block = jnp.where(line == 0, w_high.astype(f32), 0.0)
        block = jnp.where(line == 1, w_mid.astype(f32), block)
        block = jnp.where(line == 2, w_rest, block)
        basis[64:80, at] = block.astype(bf16)
        basis[80:128, at] = jnp.zeros((48, wide), bf16)
        loads[c].wait()
        term = dot_nt(basis[0:80, at], samples[:, at])
        product = term if product is None else product + term
    pl.semaphore_wait(barrier, count - 1)
    margin_slots[my_col] = product[64:65]
    for k in range(1, cols):
        margin_to(k).start()
    gram = dot_nt(basis[0:80, :], basis[...])
    gram_y = gram[16:32] + gram[48:64]
    gram_y = gram_y + pltpu.roll(gram_y, LANES - 32, 1)
    w_line = jnp.sum(gram[64:80], axis=0, keepdims=True)
    w_line = w_line + pltpu.roll(w_line, LANES - 32, 1)
    gram_slots[my_col] = gram_y
    for k in range(1, cols):
        gram_to(k).start()
    projected = product[0:32] + product[32:64]

    label_copy.wait()
    labels = labels_ref[...].astype(f32)
    for k in range(1, cols):
        margin_from(k).wait_recv()
    margin = margin_slots[0]
    for k in range(1, cols):
        margin = margin + margin_slots[k]
    resid = (jax.nn.sigmoid(margin) - labels).astype(bf16)
    resid_wide = resid.astype(f32)
    dots = jnp.sum(projected * resid_wide, axis=1, keepdims=True)
    spread = jnp.where(iota((32, LANES), 0) == iota((32, LANES), 1), dots, 0.0)
    dot_slots[my_place] = penalty * jnp.sum(spread, axis=0, keepdims=True) + w_line * (1.0 / rows)

    def dot_copy(k, owner):
        place = lax.rem(my_place + k, count)
        slot = my_place if owner else place
        return pltpu.make_async_remote_copy(
            src_ref=dot_slots.at[slot], dst_ref=dot_slots.at[slot],
            send_sem=dot_send.at[k], recv_sem=dot_recv.at[slot],
            device_id=(place // cols, lax.rem(place, cols)),
            device_id_type=pl.DeviceIdType.MESH,
        )

    for i in range(rows):
        for j in range(cols):
            if i or j:
                pltpu.make_async_remote_copy(
                    src_ref=dot_slots.at[my_place], dst_ref=dot_slots.at[my_place],
                    send_sem=dot_send.at[i * cols + j], recv_sem=dot_recv.at[my_place],
                    device_id=(lax.rem(my_row + i, rows), lax.rem(my_col + j, cols)),
                    device_id_type=pl.DeviceIdType.MESH,
                ).start()

    def total_copy(k, c, owner):
        place = lax.rem(my_row + k, rows)
        slot = my_row if owner else place
        return pltpu.make_async_remote_copy(
            src_ref=total_slots.at[slot, c], dst_ref=total_slots.at[slot, c],
            send_sem=total_send.at[k, c], recv_sem=total_recv.at[slot, c],
            device_id=(place, my_col), device_id_type=pl.DeviceIdType.MESH,
        )

    resid_rows = jnp.broadcast_to(resid_wide, (16, resid.shape[1])).astype(bf16)
    for c in range(SEND_CHUNKS):
        at = pl.ds(c * part, part)
        total = jnp.dot(resid_rows, samples[:, at], preferred_element_type=f32)
        total_slots[my_row, c] = total[0:1]
        for k in range(1, rows):
            total_copy(k, c, True).start()

    for k in range(1, cols):
        gram_from(k).wait_recv()
    gram = gram_slots[0]
    for k in range(1, cols):
        gram = gram + gram_slots[k]
    newest = lax.rem(counter_ref[0], HIST)
    line, lane = iota((HIST, LANES), 0), iota((HIST, LANES), 1)
    small = lane < HIST
    eye = line == lane
    age_line = lax.rem(newest - line + HIST, HIST)
    age_lane = lax.rem(newest - lane + LANES, HIST)
    sy = jnp.where(small, gram, 0.0)
    yy = jnp.where(small, pltpu.roll(gram, LANES - HIST, 1), 0.0)
    diagonal = jnp.where(eye, sy, 0.0)
    rho_line = 1.0 / jnp.sum(diagonal, axis=1, keepdims=True)
    diag_lane = jnp.sum(diagonal, axis=0, keepdims=True)
    rho_lane = 1.0 / jnp.where(small[0:1], diag_lane, 1.0)
    at_newest = jnp.logical_and(eye, line == newest)
    gamma = jnp.sum(
        jnp.sum(jnp.where(at_newest, sy, 0.0), axis=1, keepdims=True), axis=0, keepdims=True
    ) / jnp.sum(
        jnp.sum(jnp.where(at_newest, yy, 0.0), axis=1, keepdims=True), axis=0, keepdims=True
    )
    strict = jnp.logical_and(small, age_lane > age_line)
    factor = jnp.where(strict, sy * rho_lane, 0.0)
    solved = jnp.where(eye, 1.0, 0.0)
    columns = [
        jnp.sum(jnp.where(age_lane == age, factor, 0.0), axis=1, keepdims=True)
        for age in range(HIST)
    ]
    for age in reversed(range(1, HIST)):
        row = jnp.sum(jnp.where(age_line == age, solved, 0.0), axis=0, keepdims=True)
        solved = solved - columns[age] * row
    solved = solved * rho_line
    tall = lambda block: jnp.concatenate([block, jnp.zeros((LANES - HIST, LANES), f32)], axis=0)
    middle = diagonal + gamma * yy
    inverse = dot_nt(jnp.where(eye, 1.0, 0.0), tall(solved), highest)
    half = dot_nt(middle, tall(solved), highest)
    lower = jnp.dot(solved, tall(half), precision=highest, preferred_element_type=f32)
    map_y = -gamma * inverse
    map_s = lower - gamma * pltpu.roll(solved, HIST, 1)

    def dot_wait(k, carry):
        dot_copy(k, False).wait_recv()
        return carry

    lax.fori_loop(1, count, dot_wait, 0)
    inner = jnp.sum(dot_slots[...], axis=0)
    inner = jnp.where(iota((1, LANES), 1) < 32, inner, 0.0)
    for k in range(1, cols):
        gram_to(k).wait_send()
        margin_to(k).wait_send()

    def dot_sent(k, carry):
        dot_copy(k, True).wait_send()
        return carry

    lax.fori_loop(1, count, dot_sent, 0)
    coef_y = jnp.sum(map_y * inner, axis=1, keepdims=True)
    coef_s = jnp.sum(map_s * inner, axis=1, keepdims=True)
    for c in range(SEND_CHUNKS):
        at = pl.ds(c * part, part)
        mixed = jnp.sum(
            coef_s * hist[0:16, at] + coef_y * hist[16:32, at], axis=0, keepdims=True
        )
        for k in range(1, rows):
            total_copy(k, c, False).wait_recv()
        total = total_slots[0, c]
        for k in range(1, rows):
            total = total + total_slots[k, c]
        total = penalty * total
        grad_ref[:, at] = total
        out_ref[:, at] = -step_length * (gamma * (weights[:, at] + total) + mixed)

    for c in range(SEND_CHUNKS):
        for k in range(1, rows):
            total_copy(k, c, True).wait_send()


def body(rows, cols, samples, labels, weights, hist_s, hist_y, counter):
    height, feat = samples.shape
    count = rows * cols
    dma = pltpu.SemaphoreType.DMA
    anywhere = pl.BlockSpec(memory_space=pl.ANY)
    vmem = pl.BlockSpec(memory_space=pltpu.VMEM)
    direction, total = pl.pallas_call(
        functools.partial(kernel, rows, cols),
        out_shape=[jax.ShapeDtypeStruct((1, feat), f32)] * 2,
        in_specs=[pl.BlockSpec(memory_space=pltpu.SMEM)] + [anywhere] * 5,
        out_specs=[vmem, vmem],
        scratch_shapes=[
            pltpu.VMEM((1, height), jnp.int32),
            pltpu.VMEM((height, feat), bf16),
            pltpu.VMEM((1, feat), f32),
            pltpu.VMEM((2 * HIST, feat), f32),
            pltpu.VMEM((LANES, feat), bf16),
            pltpu.VMEM((cols, HIST, LANES), f32),
            pltpu.VMEM((cols, 1, height), f32),
            pltpu.VMEM((count, 1, LANES), f32),
            pltpu.VMEM((rows, SEND_CHUNKS, 1, feat // SEND_CHUNKS), f32),
            dma((LOAD_CHUNKS,)),
            dma((4,)),
            dma((cols,)),
            dma((cols,)),
            dma((cols,)),
            dma((cols,)),
            dma((count,)),
            dma((count,)),
            dma((rows, SEND_CHUNKS)),
            dma((rows, SEND_CHUNKS)),
        ],
        compiler_params=pltpu.CompilerParams(
            collective_id=0, has_side_effects=True, vmem_limit_bytes=60 * 1024 * 1024
        ),
    )(counter, labels.reshape(1, height), samples, weights.reshape(1, feat), hist_s, hist_y)
    direction, total = direction.reshape(feat), total.reshape(feat)
    return weights + direction, weights + total


def solution(mesh):
    in_specs = (P("rows", "cols"), P("rows"), P("cols"), P(None, "cols"), P(None, "cols"), P())
    out_specs = (P("cols"), P("cols"))
    run = functools.partial(body, mesh.shape["rows"], mesh.shape["cols"])
    return jax.shard_map(run, mesh=mesh, in_specs=in_specs, out_specs=out_specs, check_vma=False)
```
